512 devices in a mesh: ops: 64 (over y_lo, z, core), sec: 8 (over y_hi, x).
Axes of the slice: x: 4, y: 8 (y_hi: 2, y_lo: 4; y = y_hi * 4 + y_lo), z: 8, core: 2. Of those that a mesh axis runs over, the one named last changes fastest.
Arguments:
- wavefunction: bfloat16 [8, 512, 512], P('sec', 'ops'), may hold values from -6 to 6
- left_blocks: bfloat16 [8, 256, 512, 512], P('sec', 'ops'), may hold values from -0.25 to 0.25
- right_blocks: bfloat16 [8, 256, 512, 512], P('sec', 'ops'), may hold values from -0.03125 to 0.03125
- pair_index: int32 [8, 256], P('sec', 'ops'), may hold values from 0 to 3
- term_counts: int32 [8, 64], P('sec'), may hold values from 0 to 4, as said below
- charges: int32 [8], P('sec'), may hold values from 0 to 7
Outputs:
- applied: bfloat16 [8, 512, 512], P('sec', 'ops')
The draws below stay inside these ranges and needn't reach their ends.
Inputs may be any that keep to these rules, and one draw needn't show every extreme that they name: `term_counts`: in every sector exactly one device row holds 4 live terms and every other holds 0 to 2; live terms fill a device's slots from slot 0 on.
All inputs are finite; a program needn't handle non-finite values.
Results may differ from the reference program's by a relative error of at most 0.0029.
Values may be sent and summed in bfloat16 or wider, within the bound.
No kernel may reach another device: no remote copies, remote signals or barrier semaphores. Data moves between devices by JAX's collectives and lax.ppermute only.
A program may use at most 64 MiB of HBM per device.

```python
import jax
import jax.numpy as jnp
from jax import lax

M = 512
CAP = 4
SEC = 8
SLOTS = 256
N_OPS = 64


def draw_term_counts(key, part):
    base_key, spot_key = jax.random.split(jax.random.fold_in(key, 7))
    background = jax.random.randint(base_key, (SEC, N_OPS), 0, 3)
    busiest = jax.random.randint(spot_key, (SEC, 1), 0, N_OPS)
    places = jnp.arange(N_OPS, dtype=jnp.int32)[None, :]
    return jnp.where(places == busiest, CAP, background).astype(jnp.int32)


def set_ends(array, rng, smallest, largest):
    longest = array.shape.index(max(array.shape))
    spots = []
    for shift in (0, 1):
        where = [jax.random.randint(jax.random.fold_in(rng, axis), (), 0, length) for axis, length in enumerate(array.shape)]
        where[longest] = (where[longest] + shift) % array.shape[longest]
        spots.append(tuple(where))
    return array.at[spots[0]].set(smallest).at[spots[1]].set(largest)


def shard_levels(stream_key, shape, cuts, smallest, high):
    def one(axis_at, blocks):
        steps = jax.random.uniform(jax.random.fold_in(jax.random.fold_in(stream_key, 6), axis_at), (blocks,), jnp.float32, smallest / len(cuts), high / len(cuts))
        return jnp.repeat(jnp.exp(steps), shape[axis_at] // blocks).reshape((-1,) + (1,) * (len(shape) - axis_at - 1))

    loudness = one(*cuts[0])
    for cut in cuts[1:]:
        loudness = loudness * one(*cut)
    return loudness


def scatter_about(key, dims, deviation, limit, pieces=(), kind=jnp.bfloat16):
    level = shard_levels(key, dims, pieces, -0.22, 0.18) if pieces else 1.0
    values = jax.random.normal(key, dims, jnp.float32) * deviation * level
    return jnp.minimum(jnp.maximum(values, -limit), limit).astype(kind)


def setup_inputs(seed: int = 0) -> dict:
    splits = jax.random.split(jax.random.key(seed), 7)
    return {
        "wavefunction": scatter_about(splits[0], (SEC, M, M), 1.0, 6.0, ((0, 8), (1, 64))),
        "left_blocks": scatter_about(splits[1], (SEC, SLOTS, M, M), M ** -0.5, 0.25, ((0, 8), (1, 64))),
        "right_blocks": scatter_about(splits[2], (SEC, SLOTS, M, M), (M * N_OPS) ** -0.5, 0.03125, ((0, 8), (1, 64))),
        "pair_index": set_ends(jax.random.randint(splits[3], (SEC, SLOTS), 0, CAP), jax.random.fold_in(splits[3], 1), 0, CAP - 1).astype(jnp.int32),
        "term_counts": draw_term_counts(jax.random.fold_in(splits[6], 71), 0),
        "charges": set_ends(jax.random.randint(splits[5], (SEC,), 0, 8), jax.random.fold_in(splits[5], 1), 0, 7).astype(jnp.int32),
    }


def sector_terms(wavefunction, lefts, rights, pair_picks, counts):
    def add_term(running, global_slot):
        holder = global_slot // CAP
        within = global_slot % CAP

        def compute(current):
            left_block = lefts[global_slot]
            right_block = rights[holder * CAP + pair_picks[global_slot]]
            product = jnp.dot(left_block, wavefunction, preferred_element_type=jnp.float32).astype(jnp.bfloat16)
            return current + jnp.dot(product, right_block, preferred_element_type=jnp.float32)

        return lax.cond(within < counts[holder], compute, lambda current: current, running), None

    start_sum = jnp.zeros((M, M), jnp.float32)
    result, unused = lax.scan(add_term, start_sum, jnp.arange(SLOTS, dtype=jnp.int32))
    return result


def reference(wavefunction, left_blocks, right_blocks, pair_index, term_counts, charges):
    outputs = []
    carried = jnp.zeros((M, M), jnp.float32)
    for sector in range(SEC):
        onsite = 0.5 * charges[sector].astype(jnp.float32) * wavefunction[sector].astype(jnp.float32)
        outputs.append((onsite + carried).astype(jnp.bfloat16))
        if sector + 1 < SEC:
            carried = sector_terms(wavefunction[sector], left_blocks[sector], right_blocks[sector], pair_index[sector], term_counts[sector])
    return jnp.stack(outputs)
```

```python
import jax
import jax.numpy as jnp
from jax import lax
from jax.experimental import pallas as pl
from jax.experimental.pallas import tpu as pltpu
from jax.sharding import PartitionSpec as P

CORES = 2


def core_pairs(length):
    return [[chip * CORES + core for core in range(CORES)] for chip in range(length // CORES)]


def same_core(length):
    return [[chip * CORES + core for chip in range(length // CORES)] for core in range(CORES)]


def terms_kernel(psi_ref, counts_ref, picks_ref, lefts_ref, rights_ref, own_ref, other_ref,
                 left_buf, right_buf, psi_buf, acc_ref, left_sems, right_sems):
    position = lax.axis_index("ops")
    core = position % CORES
    chips, band = own_ref.shape[0], own_ref.shape[1]
    live = counts_ref[0, position]

    def left_copy(slot):
        return pltpu.make_async_copy(lefts_ref.at[0, slot], left_buf.at[slot], left_sems.at[slot])

    def right_copy(slot):
        return pltpu.make_async_copy(
            rights_ref.at[0, picks_ref[0, slot]], right_buf.at[slot], right_sems.at[slot]
        )

    for slot in range(left_buf.shape[0]):

        @pl.when(slot < live)
        def _():
            left_copy(slot).start()
            right_copy(slot).start()

    for chip in range(chips):
        for c in range(CORES):
            psi_buf[pl.ds((chip * CORES + c) * band, band), :] = psi_ref[c, chip]
    acc_ref[...] = jnp.zeros_like(acc_ref)

    def add_term(slot, carry):
        left_copy(slot).wait()
        product = jnp.dot(
            left_buf[slot], psi_buf[...], preferred_element_type=jnp.float32
        ).astype(jnp.bfloat16)
        right_copy(slot).wait()
        acc_ref[...] += jnp.dot(product, right_buf[slot], preferred_element_type=jnp.float32)
        return carry

    lax.fori_loop(0, live, add_term, 0)
    for chip in range(chips):
        mine = pl.multiple_of((chip * CORES + core) * band, band)
        theirs = pl.multiple_of((chip * CORES + 1 - core) * band, band)
        own_ref[chip] = acc_ref[pl.ds(mine, band), :]
        other_ref[chip] = acc_ref[pl.ds(theirs, band), :].astype(jnp.bfloat16)


def summed_terms(psi, term_counts, pair_index, left_blocks, right_blocks):
    chips, band, columns = psi.shape[1:]
    slots, size = left_blocks.shape[1:3]
    vmem = pl.BlockSpec(memory_space=pltpu.VMEM)
    smem = pl.BlockSpec(memory_space=pltpu.SMEM)
    hbm = pl.BlockSpec(memory_space=pltpu.HBM)
    return pl.pallas_call(
        terms_kernel,
        out_shape=(
            jax.ShapeDtypeStruct((chips, band, columns), jnp.float32),
            jax.ShapeDtypeStruct((chips, band, columns), jnp.bfloat16),
        ),
        in_specs=[vmem, smem, smem, hbm, hbm],
        out_specs=(vmem, vmem),
        scratch_shapes=[
            pltpu.VMEM((slots, size, size), jnp.bfloat16),
            pltpu.VMEM((slots, size, columns), jnp.bfloat16),
            pltpu.VMEM((size, columns), jnp.bfloat16),
            pltpu.VMEM((size, columns), jnp.float32),
            pltpu.SemaphoreType.DMA((slots,)),
            pltpu.SemaphoreType.DMA((slots,)),
        ],
        compiler_params=pltpu.CompilerParams(vmem_limit_bytes=24 * 1024 * 1024),
        name="terms",
    )(
        psi,
        pltpu.with_memory_space_constraint(term_counts, pltpu.HBM),
        pltpu.with_memory_space_constraint(pair_index, pltpu.HBM),
        pltpu.with_memory_space_constraint(left_blocks, pltpu.HBM),
        pltpu.with_memory_space_constraint(right_blocks, pltpu.HBM),
    )


def per_device(wavefunction, left_blocks, right_blocks, pair_index, term_counts, charges):
    own_rows = wavefunction[0]
    length = lax.axis_size("ops")
    chips = length // CORES
    pairs, peers = core_pairs(length), same_core(length)
    core = lax.axis_index("ops") % CORES

    copies = jnp.broadcast_to(own_rows[None], (chips, *own_rows.shape))
    bands = lax.all_to_all(copies, "ops", 0, 0, axis_index_groups=peers, tiled=True)
    psi = lax.all_gather(bands, "ops", axis_index_groups=pairs)

    own, other = summed_terms(psi, term_counts, pair_index, left_blocks, right_blocks)

    both = lax.all_gather(other, "ops", axis_index_groups=pairs)
    arrived = jnp.where(core == 0, both[1], both[0]).astype(jnp.float32)
    chip_sum = (own + arrived).astype(jnp.bfloat16)
    parts = lax.all_to_all(chip_sum, "ops", 0, 0, axis_index_groups=peers, tiled=True)
    summed = parts.astype(jnp.float32).sum(axis=0)

    sectors = lax.axis_size("sec")
    raised = lax.ppermute(summed, "sec", [(i, i + 1) for i in range(sectors - 1)])
    onsite = 0.5 * charges[0].astype(jnp.float32) * own_rows.astype(jnp.float32)
    return (onsite + raised).astype(jnp.bfloat16)[None]


def solution(mesh):
    return jax.shard_map(
        per_device,
        mesh=mesh,
        in_specs=(
            P("sec", "ops", None),
            P("sec", "ops", None, None),
            P("sec", "ops", None, None),
            P("sec", "ops"),
            P("sec", None),
            P("sec"),
        ),
        out_specs=P("sec", "ops", None),
        check_vma=False,
    )
```

```python
import jax
import jax.numpy as jnp
from jax import lax
from jax.experimental import pallas as pl
from jax.experimental.pallas import tpu as pltpu
from jax.sharding import PartitionSpec as P

CORES = 2
EARLY_RIGHTS = 2
TURNED_SECTOR = 3


def core_pairs(length):
    return [[chip * CORES + core for core in range(CORES)] for chip in range(length // CORES)]


def same_core(length):
    return [[chip * CORES + core for chip in range(length // CORES)] for core in range(CORES)]


def fetch_kernel(counts_ref, picks_ref, lefts_ref, rights_ref, left_buf, right_buf, meta_ref,
                 left_sems, right_sems):
    live = counts_ref[0, lax.axis_index("ops")]
    early = right_buf.shape[0]

    def left_copy(slot):
        return pltpu.make_async_copy(lefts_ref.at[0, slot], left_buf.at[slot], left_sems.at[slot])

    def right_copy(slot):
        return pltpu.make_async_copy(
            rights_ref.at[0, picks_ref[0, slot]], right_buf.at[slot], right_sems.at[slot]
        )

    meta_ref[0] = live
    for slot in range(left_buf.shape[0]):
        meta_ref[1 + slot] = picks_ref[0, slot]

        @pl.when(slot < live)
        def _():
            left_copy(slot).start()
            if slot < early:
                right_copy(slot).start()

    for slot in range(left_buf.shape[0]):

        @pl.when(slot < live)
        def _():
            left_copy(slot).wait()
            if slot < early:
                right_copy(slot).wait()


def fetched_blocks(term_counts, pair_index, left_blocks, right_blocks):
    smem = pl.BlockSpec(memory_space=pltpu.SMEM)
    hbm = pl.BlockSpec(memory_space=pltpu.HBM)
    vmem = pl.BlockSpec(memory_space=pltpu.VMEM)
    slots = left_blocks.shape[1]
    return pl.pallas_call(
        fetch_kernel,
        out_shape=(
            pltpu.VMEM(left_blocks.shape[1:], jnp.bfloat16),
            pltpu.VMEM((EARLY_RIGHTS, *right_blocks.shape[2:]), jnp.bfloat16),
            pltpu.SMEM((1 + slots,), jnp.int32),
        ),
        in_specs=[smem, smem, hbm, hbm],
        out_specs=(vmem, vmem, smem),
        scratch_shapes=[pltpu.SemaphoreType.DMA((slots,)), pltpu.SemaphoreType.DMA((EARLY_RIGHTS,))],
        compiler_params=pltpu.CompilerParams(vmem_limit_bytes=8 * 1024 * 1024),
        name="fetch",
    )(
        pltpu.with_memory_space_constraint(term_counts, pltpu.HBM),
        pltpu.with_memory_space_constraint(pair_index, pltpu.HBM),
        pltpu.with_memory_space_constraint(left_blocks, pltpu.HBM),
        pltpu.with_memory_space_constraint(right_blocks, pltpu.HBM),
    )


def terms_kernel(psi_ref, meta_ref, lefts_ref, early_ref, rights_ref, own_ref, other_ref, core_ref,
                 late_buf, psi_buf, acc_ref, late_sems):
    core = lax.axis_index("ops") % CORES
    chips, band = own_ref.shape[0], own_ref.shape[1]
    slots, early = lefts_ref.shape[0], early_ref.shape[0]
    live = meta_ref[0]
    core_ref[...] = jnp.full(core_ref.shape, core, jnp.int32)

    def late_copy(slot):
        return pltpu.make_async_copy(
            rights_ref.at[0, meta_ref[1 + slot]], late_buf.at[slot - early], late_sems.at[slot - early]
        )

    for slot in range(early, slots):

        @pl.when(slot < live)
        def _():
            late_copy(slot).start()

    for chip in range(chips):
        for c in range(CORES):
            psi_buf[pl.ds((chip * CORES + c) * band, band), :] = psi_ref[c, chip]
    acc_ref[...] = jnp.zeros_like(acc_ref)

    def add_term(slot, right_block):
        product = jnp.dot(
            lefts_ref[slot], psi_buf[...], preferred_element_type=jnp.float32
        ).astype(jnp.bfloat16)
        acc_ref[...] += jnp.dot(product, right_block(), preferred_element_type=jnp.float32)

    def early_term(slot, carry):
        add_term(slot, lambda: early_ref[slot])
        return carry

    def late_term(slot, carry):
        late_copy(slot).wait()
        add_term(slot, lambda: late_buf[slot - early])
        return carry

    lax.fori_loop(0, jnp.minimum(live, early), early_term, 0)
    lax.fori_loop(early, live, late_term, 0)
    turn = jnp.where(lax.axis_index("sec") == TURNED_SECTOR, chips // 2, 0)
    for chip in range(chips):
        mine = pl.multiple_of((chip * CORES + core) * band, band)
        theirs = pl.multiple_of((chip * CORES + 1 - core) * band, band)
        owner = lax.rem(chip + turn, chips)
        own_ref[owner] = acc_ref[pl.ds(mine, band), :]
        other_ref[owner] = acc_ref[pl.ds(theirs, band), :].astype(jnp.bfloat16)


def summed_terms(psi, meta, lefts, early_rights, right_blocks):
    chips, band, columns = psi.shape[1:]
    slots, size = lefts.shape[:2]
    late = slots - EARLY_RIGHTS
    vmem = pl.BlockSpec(memory_space=pltpu.VMEM)
    smem = pl.BlockSpec(memory_space=pltpu.SMEM)
    hbm = pl.BlockSpec(memory_space=pltpu.HBM)
    return pl.pallas_call(
        terms_kernel,
        out_shape=(
            jax.ShapeDtypeStruct((chips, band, columns), jnp.float32),
            jax.ShapeDtypeStruct((chips, band, columns), jnp.bfloat16),
            jax.ShapeDtypeStruct((band, columns), jnp.int32),
        ),
        in_specs=[vmem, smem, vmem, vmem, hbm],
        out_specs=(vmem, vmem, vmem),
        scratch_shapes=[
            pltpu.VMEM((late, size, columns), jnp.bfloat16),
            pltpu.VMEM((size, columns), jnp.bfloat16),
            pltpu.VMEM((size, columns), jnp.float32),
            pltpu.SemaphoreType.DMA((late,)),
        ],
        compiler_params=pltpu.CompilerParams(vmem_limit_bytes=24 * 1024 * 1024),
        name="terms",
    )(
        psi,
        meta,
        lefts,
        early_rights,
        pltpu.with_memory_space_constraint(right_blocks, pltpu.HBM),
    )


def shift_pairs(length, sectors):
    pairs = []
    for position in range(length):
        for sector in range(sectors - 1):
            turned = (position + length // 2) % length if sector == TURNED_SECTOR else position
            pairs.append((turned * sectors + sector, position * sectors + sector + 1))
    return pairs


def per_device(wavefunction, left_blocks, right_blocks, pair_index, term_counts, charges):
    own_rows = wavefunction[0]
    length, sectors = lax.axis_size("ops"), lax.axis_size("sec")
    chips = length // CORES
    pairs, peers = core_pairs(length), same_core(length)

    lefts, early_rights, meta = fetched_blocks(term_counts, pair_index, left_blocks, right_blocks)
    copies = jnp.broadcast_to(own_rows[None], (chips, *own_rows.shape))
    bands = lax.all_to_all(copies, "ops", 0, 0, axis_index_groups=peers, tiled=True)
    psi = lax.all_gather(bands, "ops", axis_index_groups=pairs)

    own, other, core = summed_terms(psi, meta, lefts, early_rights, right_blocks)

    both = lax.all_gather(other, "ops", axis_index_groups=pairs)
    arrived = jnp.where(core[None] == 0, both[1], both[0]).astype(jnp.float32)
    chip_sum = (own + arrived).astype(jnp.bfloat16)
    parts = lax.all_to_all(chip_sum, "ops", 0, 0, axis_index_groups=peers, tiled=True)
    summed = parts.astype(jnp.float32).sum(axis=0)

    raised = lax.ppermute(summed, ("ops", "sec"), shift_pairs(length, sectors))
    onsite = 0.5 * charges[0].astype(jnp.float32) * own_rows.astype(jnp.float32)
    return (onsite + raised).astype(jnp.bfloat16)[None]


def solution(mesh):
    return jax.shard_map(
        per_device,
        mesh=mesh,
        in_specs=(
            P("sec", "ops", None),
            P("sec", "ops", None, None),
            P("sec", "ops", None, None),
            P("sec", "ops"),
            P("sec", None),
            P("sec"),
        ),
        out_specs=P("sec", "ops", None),
        check_vma=False,
    )
```

```python
import jax
import jax.numpy as jnp
from jax import lax
from jax.experimental import pallas as pl
from jax.experimental.pallas import tpu as pltpu
from jax.sharding import PartitionSpec as P


CORES = 2
TURNED_SECTOR = 3


def core_pairs(length):
    return [[chip * CORES + core for core in range(CORES)] for chip in range(length // CORES)]


def same_core(length):
    return [[chip * CORES + core for chip in range(length // CORES)] for core in range(CORES)]


def to_partner(x):
    return lax.ppermute(x, "ops", [(i, i ^ 1) for i in range(lax.axis_size("ops"))])


def fetch_kernel(counts_ref, picks_ref, lefts_ref, rights_ref, left_buf, right_buf, meta_ref,
                 left_sems, right_sems):
    position = lax.axis_index("ops")
    core = position % CORES
    live = counts_ref[0, position]
    slots = left_buf.shape[0]

    def copies(slot):
        return (
            pltpu.make_async_copy(
                lefts_ref.at[slot, :, core], left_buf.at[slot], left_sems.at[slot]
            ),
            pltpu.make_async_copy(
                rights_ref.at[0, picks_ref[0, slot]], right_buf.at[slot], right_sems.at[slot]
            ),
        )

    meta_ref[0] = live
    meta_ref[1] = counts_ref[0, position + 1 - 2 * core]
    for slot in range(slots):

        @pl.when(slot < live)
        def _():
            for copy in copies(slot):
                copy.start()

    for slot in range(slots):

        @pl.when(slot < live)
        def _():
            for copy in copies(slot):
                copy.wait()


def fetched_blocks(term_counts, pair_index, lefts, right_blocks):
    smem = pl.BlockSpec(memory_space=pltpu.SMEM)
    hbm = pl.BlockSpec(memory_space=pltpu.HBM)
    vmem = pl.BlockSpec(memory_space=pltpu.VMEM)
    slots, chips, _, band, size = lefts.shape
    return pl.pallas_call(
        fetch_kernel,
        out_shape=(
            pltpu.VMEM((slots, chips, band, size), jnp.bfloat16),
            pltpu.VMEM(right_blocks.shape[1:], jnp.bfloat16),
            pltpu.SMEM((CORES,), jnp.int32),
        ),
        in_specs=[smem, smem, hbm, hbm],
        out_specs=(vmem, vmem, smem),
        scratch_shapes=[pltpu.SemaphoreType.DMA((slots,)), pltpu.SemaphoreType.DMA((slots,))],
        compiler_params=pltpu.CompilerParams(vmem_limit_bytes=8 * 1024 * 1024),
        name="fetch",
    )(
        pltpu.with_memory_space_constraint(term_counts, pltpu.HBM),
        pltpu.with_memory_space_constraint(pair_index, pltpu.HBM),
        pltpu.with_memory_space_constraint(lefts, pltpu.HBM),
        pltpu.with_memory_space_constraint(right_blocks, pltpu.HBM),
    )


def terms_kernel(psi_ref, meta_ref, lefts_ref, rights_ref, partner_lefts_ref, partner_rights_ref,
                 sum_ref, left_buf, right_buf, psi_buf, acc_ref, left_sems, right_sems):
    core = lax.axis_index("ops") % CORES
    slots, chips, band, size = lefts_ref.shape
    rows = chips * band
    own_live, partner_live = meta_ref[0], meta_ref[1]

    def left_copy(slot):
        return pltpu.make_async_copy(
            partner_lefts_ref.at[slot, :, core], left_buf.at[slot], left_sems.at[slot]
        )

    def right_copy(slot):
        return pltpu.make_async_copy(
            partner_rights_ref.at[slot], right_buf.at[slot], right_sems.at[slot]
        )

    for slot in range(slots):

        @pl.when(slot < partner_live)
        def _():
            left_copy(slot).start()
            right_copy(slot).start()

    for chip in range(chips):
        for c in range(CORES):
            psi_buf[pl.ds((chip * CORES + c) * band, band), :] = psi_ref[c, chip]
    acc_ref[...] = jnp.zeros_like(acc_ref)

    def own_term(slot, carry):
        product = jnp.dot(
            lefts_ref[slot].reshape(rows, size), psi_buf[...], preferred_element_type=jnp.float32
        ).astype(jnp.bfloat16)
        acc_ref[...] += jnp.dot(product, rights_ref[slot], preferred_element_type=jnp.float32)
        return carry

    def partner_term(slot, carry):
        left_copy(slot).wait()
        product = jnp.dot(
            left_buf[slot].reshape(rows, size), psi_buf[...], preferred_element_type=jnp.float32
        ).astype(jnp.bfloat16)
        right_copy(slot).wait()
        acc_ref[...] += jnp.dot(product, right_buf[slot], preferred_element_type=jnp.float32)
        return carry

    lax.fori_loop(0, own_live, own_term, 0)
    lax.fori_loop(0, partner_live, partner_term, 0)
    turn = jnp.where(lax.axis_index("sec") == TURNED_SECTOR, chips // 2, 0)
    for chip in range(chips):
        sum_ref[lax.rem(chip + turn, chips)] = acc_ref[pl.ds(chip * band, band), :].astype(
            jnp.bfloat16
        )


def summed_terms(psi, meta, lefts, rights, partner_lefts, partner_rights):
    slots, chips, band, size = lefts.shape
    columns = psi.shape[-1]
    vmem = pl.BlockSpec(memory_space=pltpu.VMEM)
    smem = pl.BlockSpec(memory_space=pltpu.SMEM)
    hbm = pl.BlockSpec(memory_space=pltpu.HBM)
    return pl.pallas_call(
        terms_kernel,
        out_shape=jax.ShapeDtypeStruct((chips, band, columns), jnp.bfloat16),
        in_specs=[vmem, smem, vmem, vmem, hbm, hbm],
        out_specs=vmem,
        scratch_shapes=[
            pltpu.VMEM(lefts.shape, jnp.bfloat16),
            pltpu.VMEM(rights.shape, jnp.bfloat16),
            pltpu.VMEM((size, columns), jnp.bfloat16),
            pltpu.VMEM((chips * band, columns), jnp.float32),
            pltpu.SemaphoreType.DMA((slots,)),
            pltpu.SemaphoreType.DMA((slots,)),
        ],
        compiler_params=pltpu.CompilerParams(vmem_limit_bytes=24 * 1024 * 1024),
        name="terms",
    )(
        psi,
        meta,
        lefts,
        rights,
        pltpu.with_memory_space_constraint(partner_lefts, pltpu.HBM),
        pltpu.with_memory_space_constraint(partner_rights, pltpu.HBM),
    )


def shift_pairs(length, sectors):
    pairs = []
    for position in range(length):
        for sector in range(sectors - 1):
            turned = (position + length // 2) % length if sector == TURNED_SECTOR else position
            pairs.append((turned * sectors + sector, position * sectors + sector + 1))
    return pairs


def per_device(wavefunction, left_blocks, right_blocks, pair_index, term_counts, charges):
    own_rows = wavefunction[0]
    length, sectors = lax.axis_size("ops"), lax.axis_size("sec")
    chips = length // CORES
    pairs, peers = core_pairs(length), same_core(length)

    copies = jnp.broadcast_to(own_rows[None], (chips, *own_rows.shape))
    bands = lax.all_to_all(copies, "ops", 0, 0, axis_index_groups=peers, tiled=True)

    by_band = (left_blocks.shape[1], chips, CORES, own_rows.shape[0], left_blocks.shape[3])
    lefts, rights, meta = fetched_blocks(
        term_counts, pair_index, left_blocks.reshape(by_band), right_blocks
    )
    partner_lefts = to_partner(left_blocks).reshape(by_band)
    partner_rights = to_partner(rights)

    psi = lax.all_gather(bands, "ops", axis_index_groups=pairs)
    chip_sum = summed_terms(psi, meta, lefts, rights, partner_lefts, partner_rights)
    parts = lax.all_to_all(chip_sum, "ops", 0, 0, axis_index_groups=peers, tiled=True)
    summed = parts.astype(jnp.float32).sum(axis=0)

    raised = lax.ppermute(summed, ("ops", "sec"), shift_pairs(length, sectors))
    onsite = 0.5 * charges[0].astype(jnp.float32) * own_rows.astype(jnp.float32)
    return (onsite + raised).astype(jnp.bfloat16)[None]


def solution(mesh):
    return jax.shard_map(
        per_device,
        mesh=mesh,
        in_specs=(
            P("sec", "ops", None),
            P("sec", "ops", None, None),
            P("sec", "ops", None, None),
            P("sec", "ops"),
            P("sec", None),
            P("sec"),
        ),
        out_specs=P("sec", "ops", None),
        check_vma=False,
    )
```

```python
import jax
import jax.numpy as jnp
from jax import lax
from jax.experimental import pallas as pl
from jax.experimental.pallas import tpu as pltpu
from jax.sharding import PartitionSpec as P

CORES = 2
EARLY_RIGHTS = 2
TURNED_SECTOR = 3


PEER_ORDER = (
    26, 17, 11, 10, 28, 1, 5, 4, 7, 16, 9, 19, 30, 13, 22, 0,
    21, 29, 6, 12, 20, 23, 14, 15, 3, 31, 2, 24, 25, 27, 18, 8,
)


def core_pairs(length):
    return [[chip * CORES + core for core in range(CORES)] for chip in range(length // CORES)]


def same_core(length):
    assert sorted(PEER_ORDER) == list(range(length // CORES))
    return [[chip * CORES + core for chip in PEER_ORDER] for core in range(CORES)]


def fetch_kernel(counts_ref, picks_ref, lefts_ref, rights_ref, left_buf, right_buf, meta_ref,
                 left_sems, right_sems):
    live = counts_ref[0, lax.axis_index("ops")]
    early = right_buf.shape[0]

    def left_copy(slot):
        return pltpu.make_async_copy(lefts_ref.at[0, slot], left_buf.at[slot], left_sems.at[slot])

    def right_copy(slot):
        return pltpu.make_async_copy(
            rights_ref.at[0, picks_ref[0, slot]], right_buf.at[slot], right_sems.at[slot]
        )

    meta_ref[0] = live
    for slot in range(left_buf.shape[0]):
        meta_ref[1 + slot] = picks_ref[0, slot]

        @pl.when(slot < live)
        def _():
            left_copy(slot).start()
            if slot < early:
                right_copy(slot).start()

    for slot in range(left_buf.shape[0]):

        @pl.when(slot < live)
        def _():
            left_copy(slot).wait()
            if slot < early:
                right_copy(slot).wait()


def fetched_blocks(term_counts, pair_index, left_blocks, right_blocks):
    smem = pl.BlockSpec(memory_space=pltpu.SMEM)
    hbm = pl.BlockSpec(memory_space=pltpu.HBM)
    vmem = pl.BlockSpec(memory_space=pltpu.VMEM)
    slots = left_blocks.shape[1]
    return pl.pallas_call(
        fetch_kernel,
        out_shape=(
            pltpu.VMEM(left_blocks.shape[1:], jnp.bfloat16),
            pltpu.VMEM((EARLY_RIGHTS, *right_blocks.shape[2:]), jnp.bfloat16),
            pltpu.SMEM((1 + slots,), jnp.int32),
        ),
        in_specs=[smem, smem, hbm, hbm],
        out_specs=(vmem, vmem, smem),
        scratch_shapes=[pltpu.SemaphoreType.DMA((slots,)), pltpu.SemaphoreType.DMA((EARLY_RIGHTS,))],
        compiler_params=pltpu.CompilerParams(vmem_limit_bytes=8 * 1024 * 1024),
        name="fetch",
    )(
        pltpu.with_memory_space_constraint(term_counts, pltpu.HBM),
        pltpu.with_memory_space_constraint(pair_index, pltpu.HBM),
        pltpu.with_memory_space_constraint(left_blocks, pltpu.HBM),
        pltpu.with_memory_space_constraint(right_blocks, pltpu.HBM),
    )


def terms_kernel(psi_ref, meta_ref, lefts_ref, early_ref, rights_ref, own_ref, other_ref, core_ref,
                 late_buf, psi_buf, acc_ref, late_sems):
    core = lax.axis_index("ops") % CORES
    chips, band = own_ref.shape[0], own_ref.shape[1]
    slots, early = lefts_ref.shape[0], early_ref.shape[0]
    live = meta_ref[0]
    core_ref[...] = jnp.full(core_ref.shape, core, jnp.int32)

    def late_copy(slot):
        return pltpu.make_async_copy(
            rights_ref.at[0, meta_ref[1 + slot]], late_buf.at[slot - early], late_sems.at[slot - early]
        )

    for slot in range(early, slots):

        @pl.when(slot < live)
        def _():
            late_copy(slot).start()

    for place, chip in enumerate(PEER_ORDER):
        for c in range(CORES):
            psi_buf[pl.ds((chip * CORES + c) * band, band), :] = psi_ref[c, place]
    acc_ref[...] = jnp.zeros_like(acc_ref)

    def add_term(slot, right_block):
        product = jnp.dot(
            lefts_ref[slot], psi_buf[...], preferred_element_type=jnp.float32
        ).astype(jnp.bfloat16)
        acc_ref[...] += jnp.dot(product, right_block(), preferred_element_type=jnp.float32)

    def early_term(slot, carry):
        add_term(slot, lambda: early_ref[slot])
        return carry

    def late_term(slot, carry):
        late_copy(slot).wait()
        add_term(slot, lambda: late_buf[slot - early])
        return carry

    lax.fori_loop(0, jnp.minimum(live, early), early_term, 0)
    lax.fori_loop(early, live, late_term, 0)
    turned = lax.axis_index("sec") == TURNED_SECTOR
    for chip in range(chips):
        mine = pl.multiple_of((chip * CORES + core) * band, band)
        theirs = pl.multiple_of((chip * CORES + 1 - core) * band, band)
        owner = jnp.where(
            turned,
            PEER_ORDER.index((chip + chips // 2) % chips),
            PEER_ORDER.index(chip),
        )
        own_ref[owner] = acc_ref[pl.ds(mine, band), :]
        other_ref[owner] = acc_ref[pl.ds(theirs, band), :].astype(jnp.bfloat16)


def summed_terms(psi, meta, lefts, early_rights, right_blocks):
    chips, band, columns = psi.shape[1:]
    slots, size = lefts.shape[:2]
    late = slots - EARLY_RIGHTS
    vmem = pl.BlockSpec(memory_space=pltpu.VMEM)
    smem = pl.BlockSpec(memory_space=pltpu.SMEM)
    hbm = pl.BlockSpec(memory_space=pltpu.HBM)
    return pl.pallas_call(
        terms_kernel,
        out_shape=(
            jax.ShapeDtypeStruct((chips, band, columns), jnp.float32),
            jax.ShapeDtypeStruct((chips, band, columns), jnp.bfloat16),
            jax.ShapeDtypeStruct((band, columns), jnp.int32),
        ),
        in_specs=[vmem, smem, vmem, vmem, hbm],
        out_specs=(vmem, vmem, vmem),
        scratch_shapes=[
            pltpu.VMEM((late, size, columns), jnp.bfloat16),
            pltpu.VMEM((size, columns), jnp.bfloat16),
            pltpu.VMEM((size, columns), jnp.float32),
            pltpu.SemaphoreType.DMA((late,)),
        ],
        compiler_params=pltpu.CompilerParams(vmem_limit_bytes=24 * 1024 * 1024),
        name="terms",
    )(
        psi,
        meta,
        lefts,
        early_rights,
        pltpu.with_memory_space_constraint(right_blocks, pltpu.HBM),
    )


def shift_pairs(length, sectors):
    pairs = []
    for position in range(length):
        for sector in range(sectors - 1):
            turned = (position + length // 2) % length if sector == TURNED_SECTOR else position
            pairs.append((turned * sectors + sector, position * sectors + sector + 1))
    return pairs


def per_device(wavefunction, left_blocks, right_blocks, pair_index, term_counts, charges):
    own_rows = wavefunction[0]
    length, sectors = lax.axis_size("ops"), lax.axis_size("sec")
    chips = length // CORES
    pairs, peers = core_pairs(length), same_core(length)

    lefts, early_rights, meta = fetched_blocks(term_counts, pair_index, left_blocks, right_blocks)
    copies = jnp.broadcast_to(own_rows[None], (chips, *own_rows.shape))
    bands = lax.all_to_all(copies, "ops", 0, 0, axis_index_groups=peers, tiled=True)
    psi = lax.all_gather(bands, "ops", axis_index_groups=pairs)

    own, other, core = summed_terms(psi, meta, lefts, early_rights, right_blocks)

    both = lax.all_gather(other, "ops", axis_index_groups=pairs)
    arrived = jnp.where(core[None] == 0, both[1], both[0]).astype(jnp.float32)
    chip_sum = (own + arrived).astype(jnp.bfloat16)
    parts = lax.all_to_all(chip_sum, "ops", 0, 0, axis_index_groups=peers, tiled=True)
    summed = parts.astype(jnp.float32).sum(axis=0)

    raised = lax.ppermute(summed, ("ops", "sec"), shift_pairs(length, sectors))
    onsite = 0.5 * charges[0].astype(jnp.float32) * own_rows.astype(jnp.float32)
    return (onsite + raised).astype(jnp.bfloat16)[None]


def solution(mesh):
    return jax.shard_map(
        per_device,
        mesh=mesh,
        in_specs=(
            P("sec", "ops", None),
            P("sec", "ops", None, None),
            P("sec", "ops", None, None),
            P("sec", "ops"),
            P("sec", None),
            P("sec"),
        ),
        out_specs=P("sec", "ops", None),
        check_vma=False,
    )
```

```python
import jax
import jax.numpy as jnp
from jax import lax
from jax.experimental import pallas as pl
from jax.experimental.pallas import tpu as pltpu
from jax.sharding import PartitionSpec as P


CORES = 2
TURNED_SECTOR = 3


GATHER_ORDER = (
    31, 30, 29, 28, 27, 26, 25, 24, 23, 22, 21, 20, 19, 18, 17, 16,
    15, 14, 13, 12, 11, 10, 9, 8, 7, 6, 5, 4, 3, 2, 1, 0,
)
REDUCE_ORDER = (
    19, 6, 9, 20, 24, 22, 27, 1, 10, 28, 3, 13, 2, 5, 18, 25,
    23, 17, 7, 14, 31, 15, 26, 0, 12, 4, 11, 29, 16, 21, 8, 30,
)


def core_pairs(length):
    return [[chip * CORES + core for core in range(CORES)] for chip in range(length // CORES)]


def same_core(order):
    return [[chip * CORES + core for chip in order] for core in range(CORES)]


def to_partner(x):
    return lax.ppermute(x, "ops", [(i, i ^ 1) for i in range(lax.axis_size("ops"))])


def fetch_kernel(counts_ref, picks_ref, lefts_ref, rights_ref, left_buf, right_buf, meta_ref,
                 left_sems, right_sems):
    position = lax.axis_index("ops")
    core = position % CORES
    live = counts_ref[0, position]
    slots = left_buf.shape[0]

    def copies(slot):
        return (
            pltpu.make_async_copy(
                lefts_ref.at[slot, :, core], left_buf.at[slot], left_sems.at[slot]
            ),
            pltpu.make_async_copy(
                rights_ref.at[0, picks_ref[0, slot]], right_buf.at[slot], right_sems.at[slot]
            ),
        )

    meta_ref[0] = live
    meta_ref[1] = counts_ref[0, position + 1 - 2 * core]
    for slot in range(slots):

        @pl.when(slot < live)
        def _():
            for copy in copies(slot):
                copy.start()

    for slot in range(slots):

        @pl.when(slot < live)
        def _():
            for copy in copies(slot):
                copy.wait()


def fetched_blocks(term_counts, pair_index, lefts, right_blocks):
    smem = pl.BlockSpec(memory_space=pltpu.SMEM)
    hbm = pl.BlockSpec(memory_space=pltpu.HBM)
    vmem = pl.BlockSpec(memory_space=pltpu.VMEM)
    slots, chips, _, band, size = lefts.shape
    return pl.pallas_call(
        fetch_kernel,
        out_shape=(
            pltpu.VMEM((slots, chips, band, size), jnp.bfloat16),
            pltpu.VMEM(right_blocks.shape[1:], jnp.bfloat16),
            pltpu.SMEM((CORES,), jnp.int32),
        ),
        in_specs=[smem, smem, hbm, hbm],
        out_specs=(vmem, vmem, smem),
        scratch_shapes=[pltpu.SemaphoreType.DMA((slots,)), pltpu.SemaphoreType.DMA((slots,))],
        compiler_params=pltpu.CompilerParams(vmem_limit_bytes=8 * 1024 * 1024),
        name="fetch",
    )(
        pltpu.with_memory_space_constraint(term_counts, pltpu.HBM),
        pltpu.with_memory_space_constraint(pair_index, pltpu.HBM),
        pltpu.with_memory_space_constraint(lefts, pltpu.HBM),
        pltpu.with_memory_space_constraint(right_blocks, pltpu.HBM),
    )


def terms_kernel(psi_ref, meta_ref, lefts_ref, rights_ref, partner_lefts_ref, partner_rights_ref,
                 sum_ref, left_buf, right_buf, psi_buf, acc_ref, left_sems, right_sems):
    core = lax.axis_index("ops") % CORES
    slots, chips, band, size = lefts_ref.shape
    rows = chips * band
    own_live, partner_live = meta_ref[0], meta_ref[1]

    def left_copy(slot):
        return pltpu.make_async_copy(
            partner_lefts_ref.at[slot, :, core], left_buf.at[slot], left_sems.at[slot]
        )

    def right_copy(slot):
        return pltpu.make_async_copy(
            partner_rights_ref.at[slot], right_buf.at[slot], right_sems.at[slot]
        )

    for slot in range(slots):

        @pl.when(slot < partner_live)
        def _():
            left_copy(slot).start()
            right_copy(slot).start()

    for place, chip in enumerate(GATHER_ORDER):
        for c in range(CORES):
            psi_buf[pl.ds((chip * CORES + c) * band, band), :] = psi_ref[c, place]
    acc_ref[...] = jnp.zeros_like(acc_ref)

    def own_term(slot, carry):
        product = jnp.dot(
            lefts_ref[slot].reshape(rows, size), psi_buf[...], preferred_element_type=jnp.float32
        ).astype(jnp.bfloat16)
        acc_ref[...] += jnp.dot(product, rights_ref[slot], preferred_element_type=jnp.float32)
        return carry

    def partner_term(slot, carry):
        left_copy(slot).wait()
        product = jnp.dot(
            left_buf[slot].reshape(rows, size), psi_buf[...], preferred_element_type=jnp.float32
        ).astype(jnp.bfloat16)
        right_copy(slot).wait()
        acc_ref[...] += jnp.dot(product, right_buf[slot], preferred_element_type=jnp.float32)
        return carry

    lax.fori_loop(0, own_live, own_term, 0)
    lax.fori_loop(0, partner_live, partner_term, 0)
    turned = lax.axis_index("sec") == TURNED_SECTOR
    for chip in range(chips):
        owner = jnp.where(
            turned,
            REDUCE_ORDER.index((chip + chips // 2) % chips),
            REDUCE_ORDER.index(chip),
        )
        sum_ref[owner] = acc_ref[pl.ds(chip * band, band), :].astype(
            jnp.bfloat16
        )


def summed_terms(psi, meta, lefts, rights, partner_lefts, partner_rights):
    slots, chips, band, size = lefts.shape
    columns = psi.shape[-1]
    vmem = pl.BlockSpec(memory_space=pltpu.VMEM)
    smem = pl.BlockSpec(memory_space=pltpu.SMEM)
    hbm = pl.BlockSpec(memory_space=pltpu.HBM)
    return pl.pallas_call(
        terms_kernel,
        out_shape=jax.ShapeDtypeStruct((chips, band, columns), jnp.bfloat16),
        in_specs=[vmem, smem, vmem, vmem, hbm, hbm],
        out_specs=vmem,
        scratch_shapes=[
            pltpu.VMEM(lefts.shape, jnp.bfloat16),
            pltpu.VMEM(rights.shape, jnp.bfloat16),
            pltpu.VMEM((size, columns), jnp.bfloat16),
            pltpu.VMEM((chips * band, columns), jnp.float32),
            pltpu.SemaphoreType.DMA((slots,)),
            pltpu.SemaphoreType.DMA((slots,)),
        ],
        compiler_params=pltpu.CompilerParams(vmem_limit_bytes=24 * 1024 * 1024),
        name="terms",
    )(
        psi,
        meta,
        lefts,
        rights,
        pltpu.with_memory_space_constraint(partner_lefts, pltpu.HBM),
        pltpu.with_memory_space_constraint(partner_rights, pltpu.HBM),
    )


def shift_pairs(length, sectors):
    pairs = []
    for position in range(length):
        for sector in range(sectors - 1):
            turned = (position + length // 2) % length if sector == TURNED_SECTOR else position
            pairs.append((turned * sectors + sector, position * sectors + sector + 1))
    return pairs


def per_device(wavefunction, left_blocks, right_blocks, pair_index, term_counts, charges):
    own_rows = wavefunction[0]
    length, sectors = lax.axis_size("ops"), lax.axis_size("sec")
    chips = length // CORES
    pairs = core_pairs(length)

    copies = jnp.broadcast_to(own_rows[None], (chips, *own_rows.shape))
    bands = lax.all_to_all(copies, "ops", 0, 0, axis_index_groups=same_core(GATHER_ORDER), tiled=True)

    by_band = (left_blocks.shape[1], chips, CORES, own_rows.shape[0], left_blocks.shape[3])
    lefts, rights, meta = fetched_blocks(
        term_counts, pair_index, left_blocks.reshape(by_band), right_blocks
    )
    partner_lefts = to_partner(left_blocks).reshape(by_band)
    partner_rights = to_partner(rights)

    psi = lax.all_gather(bands, "ops", axis_index_groups=pairs)
    chip_sum = summed_terms(psi, meta, lefts, rights, partner_lefts, partner_rights)
    parts = lax.all_to_all(chip_sum, "ops", 0, 0, axis_index_groups=same_core(REDUCE_ORDER), tiled=True)
    summed = parts.astype(jnp.float32).sum(axis=0)

    raised = lax.ppermute(summed, ("ops", "sec"), shift_pairs(length, sectors))
    onsite = 0.5 * charges[0].astype(jnp.float32) * own_rows.astype(jnp.float32)
    return (onsite + raised).astype(jnp.bfloat16)[None]


def solution(mesh):
    return jax.shard_map(
        per_device,
        mesh=mesh,
        in_specs=(
            P("sec", "ops", None),
            P("sec", "ops", None, None),
            P("sec", "ops", None, None),
            P("sec", "ops"),
            P("sec", None),
            P("sec"),
        ),
        out_specs=P("sec", "ops", None),
        check_vma=False,
    )
```

```python
import jax
import jax.numpy as jnp
from jax import lax
from jax.experimental import pallas as pl
from jax.experimental.pallas import tpu as pltpu
from jax.sharding import PartitionSpec as P


CORES = 2
PIECES = 4
TURNED_SECTOR = 3


GATHER_ORDER = (
    31, 30, 29, 28, 27, 26, 25, 24, 23, 22, 21, 20, 19, 18, 17, 16,
    15, 14, 13, 12, 11, 10, 9, 8, 7, 6, 5, 4, 3, 2, 1, 0,
)
REDUCE_ORDER = (
    19, 6, 9, 20, 24, 22, 27, 1, 10, 28, 3, 13, 2, 5, 18, 25,
    23, 17, 7, 14, 31, 15, 26, 0, 12, 4, 11, 29, 16, 21, 8, 30,
)


def core_pairs(length):
    return [[chip * CORES + core for core in range(CORES)] for chip in range(length // CORES)]


def same_core(order):
    return [[chip * CORES + core for chip in order] for core in range(CORES)]


def to_partner(x):
    return lax.ppermute(x, "ops", [(i, i ^ 1) for i in range(lax.axis_size("ops"))])


def fetch_kernel(counts_ref, picks_ref, lefts_ref, rights_ref, left_buf, right_buf, meta_ref,
                 left_sems, right_sems):
    position = lax.axis_index("ops")
    core = position % CORES
    live = counts_ref[0, position]
    slots = left_buf.shape[0]

    def copies(slot):
        return (
            pltpu.make_async_copy(
                lefts_ref.at[slot, :, core], left_buf.at[slot], left_sems.at[slot]
            ),
            pltpu.make_async_copy(
                rights_ref.at[0, picks_ref[0, slot]], right_buf.at[slot], right_sems.at[slot]
            ),
        )

    meta_ref[0] = live
    meta_ref[1] = counts_ref[0, position + 1 - 2 * core]
    for slot in range(slots):

        @pl.when(slot < live)
        def _():
            for copy in copies(slot):
                copy.start()

    for slot in range(slots):

        @pl.when(slot < live)
        def _():
            for copy in copies(slot):
                copy.wait()


def fetched_blocks(term_counts, pair_index, lefts, right_blocks):
    smem = pl.BlockSpec(memory_space=pltpu.SMEM)
    hbm = pl.BlockSpec(memory_space=pltpu.HBM)
    vmem = pl.BlockSpec(memory_space=pltpu.VMEM)
    slots, chips, _, band, size = lefts.shape
    return pl.pallas_call(
        fetch_kernel,
        out_shape=(
            pltpu.VMEM((slots, chips, band, size), jnp.bfloat16),
            pltpu.VMEM(right_blocks.shape[1:], jnp.bfloat16),
            pltpu.SMEM((CORES,), jnp.int32),
        ),
        in_specs=[smem, smem, hbm, hbm],
        out_specs=(vmem, vmem, smem),
        scratch_shapes=[pltpu.SemaphoreType.DMA((slots,)), pltpu.SemaphoreType.DMA((slots,))],
        compiler_params=pltpu.CompilerParams(vmem_limit_bytes=8 * 1024 * 1024),
        name="fetch",
    )(
        pltpu.with_memory_space_constraint(term_counts, pltpu.HBM),
        pltpu.with_memory_space_constraint(pair_index, pltpu.HBM),
        pltpu.with_memory_space_constraint(lefts, pltpu.HBM),
        pltpu.with_memory_space_constraint(right_blocks, pltpu.HBM),
    )


def terms_kernel(psi_ref, meta_ref, lefts_ref, rights_ref, partner_lefts_ref, partner_rights_ref,
                 sum_ref, left_buf, right_buf, psi_buf, acc_ref, left_sems, right_sems):
    core = lax.axis_index("ops") % CORES
    slots, chips, band, size = lefts_ref.shape
    rows = chips * band
    own_live, partner_live = meta_ref[0], meta_ref[1]

    def left_copy(slot):
        return pltpu.make_async_copy(
            partner_lefts_ref.at[slot, :, core], left_buf.at[slot], left_sems.at[slot]
        )

    def right_copy(slot):
        return pltpu.make_async_copy(
            partner_rights_ref.at[slot], right_buf.at[slot], right_sems.at[slot]
        )

    for slot in range(slots):

        @pl.when(slot < partner_live)
        def _():
            for piece in range(PIECES):
                part = pl.ds(piece * (chips // PIECES), chips // PIECES)
                pltpu.make_async_copy(
                    partner_lefts_ref.at[slot, part, core],
                    left_buf.at[slot, part],
                    left_sems.at[slot],
                ).start()
            for piece in range(PIECES):
                part = pl.ds(piece * (size // PIECES), size // PIECES)
                pltpu.make_async_copy(
                    partner_rights_ref.at[slot, part],
                    right_buf.at[slot, part],
                    right_sems.at[slot],
                ).start()

    for place, chip in enumerate(GATHER_ORDER):
        for c in range(CORES):
            psi_buf[pl.ds((chip * CORES + c) * band, band), :] = psi_ref[c, place]
    acc_ref[...] = jnp.zeros_like(acc_ref)

    def own_term(slot, carry):
        product = jnp.dot(
            lefts_ref[slot].reshape(rows, size), psi_buf[...], preferred_element_type=jnp.float32
        ).astype(jnp.bfloat16)
        acc_ref[...] += jnp.dot(product, rights_ref[slot], preferred_element_type=jnp.float32)
        return carry

    def partner_term(slot, carry):
        left_copy(slot).wait()
        product = jnp.dot(
            left_buf[slot].reshape(rows, size), psi_buf[...], preferred_element_type=jnp.float32
        ).astype(jnp.bfloat16)
        right_copy(slot).wait()
        acc_ref[...] += jnp.dot(product, right_buf[slot], preferred_element_type=jnp.float32)
        return carry

    lax.fori_loop(0, own_live, own_term, 0)
    lax.fori_loop(0, partner_live, partner_term, 0)
    turned = lax.axis_index("sec") == TURNED_SECTOR
    for chip in range(chips):
        owner = jnp.where(
            turned,
            REDUCE_ORDER.index((chip + chips // 2) % chips),
            REDUCE_ORDER.index(chip),
        )
        sum_ref[owner] = acc_ref[pl.ds(chip * band, band), :].astype(
            jnp.bfloat16
        )


def summed_terms(psi, meta, lefts, rights, partner_lefts, partner_rights):
    slots, chips, band, size = lefts.shape
    columns = psi.shape[-1]
    vmem = pl.BlockSpec(memory_space=pltpu.VMEM)
    smem = pl.BlockSpec(memory_space=pltpu.SMEM)
    hbm = pl.BlockSpec(memory_space=pltpu.HBM)
    return pl.pallas_call(
        terms_kernel,
        out_shape=jax.ShapeDtypeStruct((chips, band, columns), jnp.bfloat16),
        in_specs=[vmem, smem, vmem, vmem, hbm, hbm],
        out_specs=vmem,
        scratch_shapes=[
            pltpu.VMEM(lefts.shape, jnp.bfloat16),
            pltpu.VMEM(rights.shape, jnp.bfloat16),
            pltpu.VMEM((size, columns), jnp.bfloat16),
            pltpu.VMEM((chips * band, columns), jnp.float32),
            pltpu.SemaphoreType.DMA((slots,)),
            pltpu.SemaphoreType.DMA((slots,)),
        ],
        compiler_params=pltpu.CompilerParams(vmem_limit_bytes=24 * 1024 * 1024),
        name="terms",
    )(
        psi,
        meta,
        lefts,
        rights,
        pltpu.with_memory_space_constraint(partner_lefts, pltpu.HBM),
        pltpu.with_memory_space_constraint(partner_rights, pltpu.HBM),
    )


def shift_pairs(length, sectors):
    pairs = []
    for position in range(length):
        for sector in range(sectors - 1):
            turned = (position + length // 2) % length if sector == TURNED_SECTOR else position
            pairs.append((turned * sectors + sector, position * sectors + sector + 1))
    return pairs


def per_device(wavefunction, left_blocks, right_blocks, pair_index, term_counts, charges):
    own_rows = wavefunction[0]
    length, sectors = lax.axis_size("ops"), lax.axis_size("sec")
    chips = length // CORES
    pairs = core_pairs(length)

    copies = jnp.broadcast_to(own_rows[None], (chips, *own_rows.shape))
    bands = lax.all_to_all(copies, "ops", 0, 0, axis_index_groups=same_core(GATHER_ORDER), tiled=True)

    by_band = (left_blocks.shape[1], chips, CORES, own_rows.shape[0], left_blocks.shape[3])
    lefts, rights, meta = fetched_blocks(
        term_counts, pair_index, left_blocks.reshape(by_band), right_blocks
    )
    partner_lefts = to_partner(left_blocks).reshape(by_band)
    partner_rights = to_partner(rights)

    psi = lax.all_gather(bands, "ops", axis_index_groups=pairs)
    chip_sum = summed_terms(psi, meta, lefts, rights, partner_lefts, partner_rights)
    parts = lax.all_to_all(chip_sum, "ops", 0, 0, axis_index_groups=same_core(REDUCE_ORDER), tiled=True)
    summed = parts.astype(jnp.float32).sum(axis=0)

    raised = lax.ppermute(summed, ("ops", "sec"), shift_pairs(length, sectors))
    onsite = 0.5 * charges[0].astype(jnp.float32) * own_rows.astype(jnp.float32)
    return (onsite + raised).astype(jnp.bfloat16)[None]


def solution(mesh):
    return jax.shard_map(
        per_device,
        mesh=mesh,
        in_specs=(
            P("sec", "ops", None),
            P("sec", "ops", None, None),
            P("sec", "ops", None, None),
            P("sec", "ops"),
            P("sec", None),
            P("sec"),
        ),
        out_specs=P("sec", "ops", None),
        check_vma=False,
    )
```
